32 devices in a mesh: dp: 4 (over x, y), tp: 8 (over z, core).
Axes of the slice: x: 2, y: 2, z: 4, core: 2. Of those that a mesh axis runs over, the one named last changes fastest.
Arguments:
- hidden: bfloat16 [4, 3072, 3072], P('dp', 'tp'), parts along dimension 0
- targets: int32 [4, 3072], P('dp', 'tp'), parts along dimension 0
- norm_gain: bfloat16 [3072], replicated
- head_w: bfloat16 [128256, 3072], P('tp')
- temperature: float32 [], replicated
Outputs:
- output 1: float32 [4, 3072], P('dp', 'tp'), parts along dimension 0
- output 2: float32 [4, 3072], P('dp', 'tp'), parts along dimension 0
There are 4 independent parts. The reference program is written for one: setup_inputs(seed, part) draws one part's arguments, and reference() takes and returns one part's arrays. A program takes and returns all parts, laid end to end along the dimension named above; an argument that names none is the same for every part.
All inputs are finite; a program needn't handle non-finite values.
Results may differ from the reference program's by a relative error of at most 0.001.
Values are sent between devices in bfloat16 or wider.
A program may use at most 1 GiB of HBM per device.

```python
import jax
import jax.numpy as jnp
from jax import lax

ROW_COUNT = 1
SEQ_LEN = 3072
BLOCK_TOKENS = 384
MODEL_DIM = 3072
VOCAB_SIZE = 128256
NORM_EPS = 1e-6
PEAK_SCALE = 10.0


def setup_inputs(seed: int = 0, part: int = 0) -> dict:
    base_key = jax.random.key(seed)
    part_key = jax.random.fold_in(base_key, part)
    key_head, key_gain, key_temp = jax.random.split(base_key, 3)
    key_noise, key_peak, key_coin, key_spread = jax.random.split(part_key, 4)
    head_wide = jax.random.normal(key_head, (VOCAB_SIZE, MODEL_DIM), jnp.float32) * MODEL_DIM ** -0.5
    gain_wide = 1.0 + 0.3 * jax.random.normal(key_gain, (MODEL_DIM,), jnp.float32)
    temperature = jax.random.uniform(key_temp, (), jnp.float32, 0.6, 0.9)
    peak_ids = jax.random.randint(key_peak, (ROW_COUNT, SEQ_LEN), 0, VOCAB_SIZE)
    noise_part = jax.random.normal(key_noise, (ROW_COUNT, SEQ_LEN, MODEL_DIM), jnp.float32)
    hidden = noise_part + PEAK_SCALE * head_wide[peak_ids]
    coin_flip = jax.random.randint(key_coin, (ROW_COUNT, SEQ_LEN), 0, 2)
    spread_ids = jax.random.randint(key_spread, (ROW_COUNT, SEQ_LEN), 0, VOCAB_SIZE)
    targets = jnp.where(coin_flip == 1, peak_ids, spread_ids).astype(jnp.int32)
    return dict(hidden=hidden.astype(jnp.bfloat16), targets=targets, norm_gain=gain_wide.astype(jnp.bfloat16), head_w=head_wide.astype(jnp.bfloat16), temperature=temperature)


def reference(hidden, targets, norm_gain, head_w, temperature):
    h_wide = hidden.astype(jnp.float32)
    inv_rms = lax.rsqrt(jnp.mean(h_wide * h_wide, axis=-1, keepdims=True) + NORM_EPS)
    normed = (norm_gain.astype(jnp.float32) * h_wide * inv_rms).astype(jnp.bfloat16)
    block_count = ROW_COUNT * SEQ_LEN // BLOCK_TOKENS
    row_blocks = normed.reshape(block_count, BLOCK_TOKENS, MODEL_DIM)
    target_blocks = targets.reshape(block_count, BLOCK_TOKENS)

    def block_stats(pair):
        rows_blk, target_blk = pair
        logits = jnp.dot(rows_blk, head_w.T, preferred_element_type=jnp.float32) / temperature
        top_val = jnp.max(logits, axis=-1, keepdims=True)
        exp_shift = jnp.exp(logits - top_val)
        sum_exp = jnp.sum(exp_shift, axis=-1)
        weighted = jnp.sum(exp_shift * logits, axis=-1)
        log_norm = top_val[:, 0] + jnp.log(sum_exp)
        target_logit = jnp.take_along_axis(logits, target_blk[:, None], axis=-1)[:, 0]
        return target_logit - log_norm, log_norm - weighted / sum_exp

    log_prob, entropy = lax.map(block_stats, (row_blocks, target_blocks))
    return log_prob.reshape(ROW_COUNT, SEQ_LEN), entropy.reshape(ROW_COUNT, SEQ_LEN)
```

```python
import functools

import jax
import jax.numpy as jnp
from jax import lax
from jax.experimental import pallas as pl
from jax.experimental.pallas import tpu as pltpu
from jax.sharding import PartitionSpec as P

NORM_EPS = 1e-6
F32 = jnp.float32
LANES = 128
SPLITS = (672, 672, 672, 656)
GROUP = 64
CHIPS = 4
CORES = 2
PEERS = CHIPS * CORES
FORWARD_TRIPS = (5, 10, 15)
MESH = pl.DeviceIdType.MESH


def _tree(op, values):
    while len(values) > 1:
        paired = [op(a, b) for a, b in zip(values[::2], values[1::2])]
        values = paired + values[len(values) & ~1:]
    return values[0]


def _xor(a, b):
    return (a % 2 + b % 2) % 2 + 2 * ((a // 2 + b // 2) % 2)


def _online(z_ref, rows, inv_tau, first_id, target, stats, cols, width):
    m_ref, s_ref, w_ref, t_ref = stats
    m, s, w, t = m_ref[:, cols], s_ref[:, cols], w_ref[:, cols], t_ref[:, cols]
    rel = target - first_id - lax.broadcasted_iota(jnp.int32, (8, width), 0)
    for r0 in range(0, rows, GROUP):
        n = min(GROUP, rows - r0)
        block = z_ref[r0:r0 + n, :] * inv_tau
        z = [block[i:i + 8] for i in range(0, n, 8)]
        m_new = jnp.maximum(m, _tree(jnp.maximum, z))
        keep = jnp.exp(m - m_new)
        p = [jnp.exp(v - m_new) for v in z]
        s = s * keep + _tree(jnp.add, p)
        w = w * keep + _tree(jnp.add, [a * b for a, b in zip(p, z)])
        for i, v in enumerate(z):
            t = jnp.where(rel == r0 + 8 * i, v, t)
        m = m_new
    m_ref[:, cols], s_ref[:, cols], w_ref[:, cols], t_ref[:, cols] = m, s, w, t


def _kernel(tok, vocab, depth, tau_ref, h_hbm, tgt_hbm, gain_ref, w_hbm, logp_ref, ent_ref,
            xs, wbuf, z0, z1, z2, z3, tgt_all, m_ref, s_ref, w_ref, t_ref, part, landed,
            h_sem, t_sem, w_sem, own_send, own_recv, recv, send_p, send_r, send_l, tgt_send, tgt_recv, st_send, st_recv):
    zs = (z0, z1, z2, z3)
    stats = (m_ref, s_ref, w_ref, t_ref)
    me = lax.axis_index('tp')
    chip, core = me // CORES, me % CORES
    other = me + 1 - 2 * core
    right, left = (me + CORES) % PEERS, (me + PEERS - CORES) % PEERS
    rows = sum(SPLITS)
    chunks = vocab // rows
    width = CORES * tok
    tiles = tok // LANES
    trips = CHIPS * chunks
    offs = [sum(SPLITS[:i]) for i in range(len(SPLITS))]
    last = len(SPLITS) - 1

    def load_h(i):
        r = pl.ds(i * LANES, LANES)
        return pltpu.make_async_copy(h_hbm.at[r], wbuf.at[1, r], h_sem.at[i])

    def load_w(t, slot):
        r = pl.ds(pl.multiple_of((t % chunks) * rows, 16), rows)
        return pltpu.make_async_copy(w_hbm.at[r], wbuf.at[slot], w_sem.at[slot])

    def block_at(b):
        return xs.at[pl.ds(b * tiles, tiles)]

    def hop(b, dst, sems):
        return pltpu.make_async_remote_copy(
            src_ref=block_at(b), dst_ref=block_at(b), send_sem=sems.at[b], recv_sem=recv.at[b],
            device_id={'tp': dst}, device_id_type=MESH)

    def own_piece(i, b):
        piece = xs.at[b * tiles + i]
        return pltpu.make_async_remote_copy(
            src_ref=piece, dst_ref=piece, send_sem=own_send.at[i], recv_sem=own_recv.at[i],
            device_id={'tp': other}, device_id_type=MESH)

    def tgt_cols(b):
        return pl.ds(pl.multiple_of(b * tok, LANES), tok)

    def send_tgt(d, b):
        c = tgt_all.at[:, tgt_cols(b)]
        return pltpu.make_async_remote_copy(
            src_ref=c, dst_ref=c, send_sem=tgt_send.at[d], recv_sem=tgt_recv.at[d],
            device_id={'tp': (me + d) % PEERS}, device_id_type=MESH)

    def send_stat(d, src, slot):
        return pltpu.make_async_remote_copy(
            src_ref=part.at[src], dst_ref=landed.at[slot], send_sem=st_send.at[d], recv_sem=st_recv.at[d],
            device_id={'tp': (me + d) % PEERS}, device_id_type=MESH)

    for i in range(tiles):
        load_h(i).start()
    own_tgt = pltpu.make_async_copy(tgt_hbm, tgt_all.at[:, tgt_cols(me)], t_sem)
    own_tgt.start()
    load_w(0, 0).start()
    barrier = pltpu.get_barrier_semaphore()
    for d in range(1, PEERS):
        pl.semaphore_signal(barrier, inc=1, device_id={'tp': (me + d) % PEERS}, device_id_type=MESH)

    inv_tau = 1.0 / tau_ref[0]
    m_ref[...] = jnp.full(m_ref.shape, -jnp.inf, F32)
    for ref in (s_ref, w_ref, t_ref):
        ref[...] = jnp.zeros(ref.shape, F32)
    spare = pl.ds(CHIPS * width, width)
    tgt_all[:, spare] = jnp.full((1, width), -1, jnp.int32)
    z3[...] = jnp.zeros(z3.shape, F32)

    def normalise(i):
        load_h(i).wait()
        r = pl.ds(i * LANES, LANES)
        acc = jnp.zeros((LANES, LANES), F32)
        for k in range(depth // LANES):
            v = wbuf[1, r, k * LANES:(k + 1) * LANES].astype(F32)
            acc = acc + v * v
        inv_rms = lax.rsqrt(jnp.sum(acc, axis=-1, keepdims=True) / depth + NORM_EPS)
        for k in range(depth // LANES):
            c = slice(k * LANES, (k + 1) * LANES)
            v = gain_ref[:, c].astype(F32) * wbuf[1, r, c].astype(F32) * inv_rms
            xs[me * tiles + i, c, :] = v.astype(jnp.bfloat16).T

    normalise(0)
    pl.semaphore_wait(barrier, PEERS - 1)
    own_tgt.wait()
    for d in range(1, PEERS):
        send_tgt(d, me).start()
    for i in range(1, tiles):
        normalise(i)
        own_piece(i - 1, me).start()
    own_piece(tiles - 1, me).start()

    @pl.when(chip < CHIPS - 1)
    def _():
        hop(me, right, send_r).start()

    @pl.when(chip > 0)
    def _():
        hop(me, left, send_l).start()

    for d in range(1, PEERS):
        send_tgt(d, (me + PEERS - d) % PEERS).wait_recv()
    for i in range(tiles):
        own_piece(i, other).wait_recv()

    def pass_on(k):
        @pl.when(chip >= k)
        def _():
            b = (me + PEERS - CORES * k) % PEERS
            hop(b, right, send_r).wait_recv()
            hop(b, other, send_p).start()

            @pl.when(chip < CHIPS - 1)
            def _():
                hop(b, right, send_r).start()

        @pl.when(chip + k < CHIPS)
        def _():
            b = (me + CORES * k) % PEERS
            hop(b, left, send_l).wait_recv()
            hop(b, other, send_p).start()

            @pl.when(chip > 0)
            def _():
                hop(b, left, send_l).start()

    def take_partners(k):
        @pl.when(chip >= k)
        def _():
            hop((other + PEERS - CORES * k) % PEERS, other, send_p).wait_recv()

        @pl.when(chip + k < CHIPS)
        def _():
            hop((other + CORES * k) % PEERS, other, send_p).wait_recv()

    def dot(slot, at, i):
        x = jnp.concatenate([xs[at * CORES * tiles + j] for j in range(CORES * tiles)], axis=1)
        zs[i][...] = jnp.dot(wbuf[slot, offs[i]:offs[i] + SPLITS[i], :], x, preferred_element_type=F32)

    def fold(c, at, i):
        cols = pl.ds(pl.multiple_of(at * width, LANES), width)
        _online(zs[i], SPLITS[i], inv_tau, me * vocab + c * rows + offs[i], tgt_all[:, cols], stats, cols, width)

    def trip(t, carry):
        slot = t % 2
        p, c = t // chunks, t % chunks
        before = jnp.maximum(t - 1, 0)
        at = _xor(chip, p)
        at_before = jnp.where(t == 0, CHIPS, _xor(chip, before // chunks))
        for k in range(1, CHIPS):
            @pl.when(t == FORWARD_TRIPS[k - 1])
            def _(k=k):
                pass_on(k)

            @pl.when(t == k * chunks)
            def _(k=k):
                take_partners(k)
        load_w(t, slot).wait()

        @pl.when(t + 1 < trips)
        def _():
            load_w(t + 1, 1 - slot).start()

        for i in range(len(SPLITS)):
            dot(slot, at, i)
            if i:
                fold(c, at, i - 1)
            else:
                fold(before % chunks, at_before, last)
        return carry

    lax.fori_loop(0, trips, trip, 0)
    fold(chunks - 1, _xor(chip, CHIPS - 1), last)

    for b in range(PEERS):
        cols = slice(b * tok, (b + 1) * tok)
        m8 = m_ref[:, cols]
        m = jnp.max(m8, axis=0, keepdims=True)
        keep = jnp.exp(m8 - m)
        part[b, 0:1, :] = m
        part[b, 1:2, :] = jnp.sum(s_ref[:, cols] * keep, axis=0, keepdims=True)
        part[b, 2:3, :] = jnp.sum(w_ref[:, cols] * keep, axis=0, keepdims=True)
        part[b, 3:4, :] = jnp.sum(t_ref[:, cols], axis=0, keepdims=True)
    for d in range(1, PEERS):
        send_stat(d, (me + d) % PEERS, me).start()
    landed[me] = part[me]

    for i in range(tiles):
        own_piece(i, me).wait_send()
    for d in range(1, PEERS):
        send_tgt(d, me).wait_send()

    @pl.when(chip < CHIPS - 1)
    def _():
        hop(me, right, send_r).wait_send()

    @pl.when(chip > 0)
    def _():
        hop(me, left, send_l).wait_send()

    for k in range(1, CHIPS):
        @pl.when(chip >= k)
        def _(k=k):
            b = (me + PEERS - CORES * k) % PEERS
            hop(b, other, send_p).wait_send()

            @pl.when(chip < CHIPS - 1)
            def _():
                hop(b, right, send_r).wait_send()

        @pl.when(chip + k < CHIPS)
        def _(k=k):
            b = (me + CORES * k) % PEERS
            hop(b, other, send_p).wait_send()

            @pl.when(chip > 0)
            def _():
                hop(b, left, send_l).wait_send()

    for d in range(1, PEERS):
        send_stat(d, (me + d) % PEERS, (me + PEERS - d) % PEERS).wait()
    got = [landed[b] for b in range(PEERS)]
    m = _tree(jnp.maximum, [g[0:1] for g in got])
    keep = [jnp.exp(g[0:1] - m) for g in got]
    s = _tree(jnp.add, [g[1:2] * k for g, k in zip(got, keep)])
    w = _tree(jnp.add, [g[2:3] * k for g, k in zip(got, keep)])
    lse = m + jnp.log(s)
    logp_ref[...] = _tree(jnp.add, [g[3:4] for g in got]) - lse
    ent_ref[...] = lse - w / s


def solution(mesh):
    def device_body(h, targets, gain, head, tau):
        tok, depth = h.shape[1:]
        vocab = head.shape[0]
        width = CORES * tok
        anywhere = pl.BlockSpec(memory_space=pl.ANY)
        vmem = pl.BlockSpec(memory_space=pltpu.VMEM)
        dma = pltpu.SemaphoreType.DMA
        stat = pltpu.VMEM((8, (CHIPS + 1) * width), F32)
        return pl.pallas_call(
            functools.partial(_kernel, tok, vocab, depth),
            out_shape=[jax.ShapeDtypeStruct((1, tok), F32)] * 2,
            in_specs=[pl.BlockSpec(memory_space=pltpu.SMEM), anywhere, anywhere, vmem, anywhere],
            out_specs=[vmem, vmem],
            scratch_shapes=[
                pltpu.VMEM((PEERS * tok // LANES, depth, LANES), jnp.bfloat16),
                pltpu.VMEM((2, sum(SPLITS), depth), jnp.bfloat16),
                *[pltpu.VMEM((r, width), F32) for r in SPLITS],
                pltpu.VMEM((1, (CHIPS + 1) * width), jnp.int32),
                stat, stat, stat, stat,
                pltpu.VMEM((PEERS, 4, tok), F32),
                pltpu.VMEM((PEERS, 4, tok), F32),
                dma((tok // LANES,)), dma, dma((2,)), dma((tok // LANES,)), dma((tok // LANES,)),
                dma((PEERS,)), dma((PEERS,)), dma((PEERS,)), dma((PEERS,)),
                dma((PEERS,)), dma((PEERS,)), dma((PEERS,)), dma((PEERS,)),
            ],
            compiler_params=pltpu.CompilerParams(
                collective_id=0, has_side_effects=True, vmem_limit_bytes=67_043_328),
        )(tau.reshape(1), h.reshape(tok, depth), targets, gain.reshape(1, depth), head)

    return jax.shard_map(
        device_body,
        mesh=mesh,
        in_specs=(P('dp', 'tp', None), P('dp', 'tp'), P(), P('tp', None), P()),
        out_specs=(P('dp', 'tp'), P('dp', 'tp')),
        check_vma=False,
    )
```

```python
import functools

import jax
import jax.numpy as jnp
from jax import lax
from jax.experimental import pallas as pl
from jax.experimental.pallas import tpu as pltpu
from jax.sharding import PartitionSpec as P

NORM_EPS = 1e-6
F32 = jnp.float32
LANES = 128
SPLITS = (672, 672, 672, 656)
GROUP = 64
CHIPS = 4
CORES = 2
PEERS = CHIPS * CORES
MESH = pl.DeviceIdType.MESH


def _tree(op, values):
    while len(values) > 1:
        paired = [op(a, b) for a, b in zip(values[::2], values[1::2])]
        values = paired + values[len(values) & ~1:]
    return values[0]


def _xor(a, b):
    return (a % 2 + b % 2) % 2 + 2 * ((a // 2 + b // 2) % 2)


def _online(z_ref, rows, inv_tau, first_id, target, stats, cols, width):
    m_ref, s_ref, w_ref, t_ref = stats
    m, s, w, t = m_ref[:, cols], s_ref[:, cols], w_ref[:, cols], t_ref[:, cols]
    rel = target - first_id - lax.broadcasted_iota(jnp.int32, (8, width), 0)
    for r0 in range(0, rows, GROUP):
        n = min(GROUP, rows - r0)
        block = z_ref[r0:r0 + n, :] * inv_tau
        z = [block[i:i + 8] for i in range(0, n, 8)]
        m_new = jnp.maximum(m, _tree(jnp.maximum, z))
        keep = jnp.exp(m - m_new)
        p = [jnp.exp(v - m_new) for v in z]
        s = s * keep + _tree(jnp.add, p)
        w = w * keep + _tree(jnp.add, [a * b for a, b in zip(p, z)])
        for i, v in enumerate(z):
            t = jnp.where(rel == r0 + 8 * i, v, t)
        m = m_new
    m_ref[:, cols], s_ref[:, cols], w_ref[:, cols], t_ref[:, cols] = m, s, w, t


def _kernel(tok, vocab, depth, tau_ref, h_hbm, tgt_hbm, gain_ref, w_hbm, out_ref,
            xs, wbuf, z0, z1, z2, z3, tgt_all, m_ref, s_ref, w_ref, t_ref, part, landed,
            h_sem, t_sem, w_sem, own_send, own_recv, recv, send_p, send_r, send_l, tgt_send, tgt_recv, st_send, st_recv):
    zs = (z0, z1, z2, z3)
    stats = (m_ref, s_ref, w_ref, t_ref)
    me = lax.axis_index('tp')
    chip, core = me // CORES, me % CORES
    other = me + 1 - 2 * core
    right, left = (me + CORES) % PEERS, (me + PEERS - CORES) % PEERS
    rows = sum(SPLITS)
    chunks = vocab // rows
    width = CORES * tok
    tiles = tok // LANES
    trips = CHIPS * chunks
    offs = [sum(SPLITS[:i]) for i in range(len(SPLITS))]
    last = len(SPLITS) - 1

    def load_h(i):
        r = pl.ds(i * LANES, LANES)
        return pltpu.make_async_copy(h_hbm.at[r], wbuf.at[1, r], h_sem.at[i])

    def load_w(t, slot):
        r = pl.ds(pl.multiple_of((t % chunks) * rows, 16), rows)
        return pltpu.make_async_copy(w_hbm.at[r], wbuf.at[slot], w_sem.at[slot])

    def block_at(b):
        return xs.at[pl.ds(b * tiles, tiles)]

    def hop(b, dst, sems):
        return pltpu.make_async_remote_copy(
            src_ref=block_at(b), dst_ref=block_at(b), send_sem=sems.at[b], recv_sem=recv.at[b],
            device_id={'tp': dst}, device_id_type=MESH)

    def own_piece(i, b):
        piece = xs.at[b * tiles + i]
        return pltpu.make_async_remote_copy(
            src_ref=piece, dst_ref=piece, send_sem=own_send.at[i], recv_sem=own_recv.at[i],
            device_id={'tp': other}, device_id_type=MESH)

    def tgt_cols(b):
        return pl.ds(pl.multiple_of(b * tok, LANES), tok)

    def send_tgt(d, b):
        c = tgt_all.at[:, tgt_cols(b)]
        return pltpu.make_async_remote_copy(
            src_ref=c, dst_ref=c, send_sem=tgt_send.at[d], recv_sem=tgt_recv.at[d],
            device_id={'tp': (me + d) % PEERS}, device_id_type=MESH)

    def send_stat(d, src, slot):
        return pltpu.make_async_remote_copy(
            src_ref=part.at[src], dst_ref=landed.at[slot], send_sem=st_send.at[d], recv_sem=st_recv.at[d],
            device_id={'tp': (me + d) % PEERS}, device_id_type=MESH)

    for i in range(tiles):
        load_h(i).start()
    own_tgt = pltpu.make_async_copy(tgt_hbm, tgt_all.at[:, tgt_cols(me)], t_sem)
    own_tgt.start()
    load_w(0, 0).start()
    barrier = pltpu.get_barrier_semaphore()
    for d in range(1, PEERS):
        pl.semaphore_signal(barrier, inc=1, device_id={'tp': (me + d) % PEERS}, device_id_type=MESH)

    inv_tau = 1.0 / tau_ref[0]
    m_ref[...] = jnp.full(m_ref.shape, -jnp.inf, F32)
    for ref in (s_ref, w_ref, t_ref):
        ref[...] = jnp.zeros(ref.shape, F32)
    spare = pl.ds(CHIPS * width, width)
    tgt_all[:, spare] = jnp.full((1, width), -1, jnp.int32)
    z3[...] = jnp.zeros(z3.shape, F32)

    def normalise(i):
        load_h(i).wait()
        r = pl.ds(i * LANES, LANES)
        acc = jnp.zeros((LANES, LANES), F32)
        for k in range(depth // LANES):
            v = wbuf[1, r, k * LANES:(k + 1) * LANES].astype(F32)
            acc = acc + v * v
        inv_rms = lax.rsqrt(jnp.sum(acc, axis=-1, keepdims=True) / depth + NORM_EPS)
        for k in range(depth // LANES):
            c = slice(k * LANES, (k + 1) * LANES)
            v = gain_ref[c].astype(F32).reshape(1, LANES) * wbuf[1, r, c].astype(F32) * inv_rms
            xs[me * tiles + i, c, :] = v.astype(jnp.bfloat16).T

    normalise(0)
    pl.semaphore_wait(barrier, PEERS - 1)
    own_tgt.wait()
    for d in range(1, PEERS):
        send_tgt(d, me).start()
    for i in range(1, tiles):
        normalise(i)
        own_piece(i - 1, me).start()
    own_piece(tiles - 1, me).start()

    @pl.when(chip < CHIPS - 1)
    def _():
        hop(me, right, send_r).start()

    @pl.when(chip > 0)
    def _():
        hop(me, left, send_l).start()

    for d in range(1, PEERS):
        send_tgt(d, (me + PEERS - d) % PEERS).wait_recv()
    for i in range(tiles):
        own_piece(i, other).wait_recv()

    def pass_on(k):
        @pl.when(chip >= k)
        def _():
            b = (me + PEERS - CORES * k) % PEERS
            hop(b, right, send_r).wait_recv()
            hop(b, other, send_p).start()

            @pl.when(chip < CHIPS - 1)
            def _():
                hop(b, right, send_r).start()

        @pl.when(chip + k < CHIPS)
        def _():
            b = (me + CORES * k) % PEERS
            hop(b, left, send_l).wait_recv()
            hop(b, other, send_p).start()

            @pl.when(chip > 0)
            def _():
                hop(b, left, send_l).start()

    def take_partners(k):
        @pl.when(chip >= k)
        def _():
            hop((other + PEERS - CORES * k) % PEERS, other, send_p).wait_recv()

        @pl.when(chip + k < CHIPS)
        def _():
            hop((other + CORES * k) % PEERS, other, send_p).wait_recv()

    def dot(slot, at, i):
        x = jnp.concatenate([xs[at * CORES * tiles + j] for j in range(CORES * tiles)], axis=1)
        zs[i][...] = jnp.dot(wbuf[slot, offs[i]:offs[i] + SPLITS[i], :], x, preferred_element_type=F32)

    def fold(c, at, i):
        cols = pl.ds(pl.multiple_of(at * width, LANES), width)
        _online(zs[i], SPLITS[i], inv_tau, me * vocab + c * rows + offs[i], tgt_all[:, cols], stats, cols, width)

    def trip(t, carry):
        slot = t % 2
        p, c = t // chunks, t % chunks
        before = jnp.maximum(t - 1, 0)
        at = _xor(chip, p)
        at_before = jnp.where(t == 0, CHIPS, _xor(chip, before // chunks))

        @pl.when((c == 0) & (p > 0))
        def _():
            take_partners(p)

        @pl.when((c == chunks - 1) & (p < CHIPS - 1))
        def _():
            pass_on(p + 1)

        load_w(t, slot).wait()

        @pl.when(t + 1 < trips)
        def _():
            load_w(t + 1, 1 - slot).start()

        for i in range(len(SPLITS)):
            dot(slot, at, i)
            if i:
                fold(c, at, i - 1)
            else:
                fold(before % chunks, at_before, last)
        return carry

    lax.fori_loop(0, trips, trip, 0)
    fold(chunks - 1, _xor(chip, CHIPS - 1), last)

    for b in range(PEERS):
        cols = slice(b * tok, (b + 1) * tok)
        m8 = m_ref[:, cols]
        m = jnp.max(m8, axis=0, keepdims=True)
        keep = jnp.exp(m8 - m)
        part[b, 0:1, :] = m
        part[b, 1:2, :] = jnp.sum(s_ref[:, cols] * keep, axis=0, keepdims=True)
        part[b, 2:3, :] = jnp.sum(w_ref[:, cols] * keep, axis=0, keepdims=True)
        part[b, 3:4, :] = jnp.sum(t_ref[:, cols], axis=0, keepdims=True)
    for d in range(1, PEERS):
        send_stat(d, (me + d) % PEERS, me).start()
    landed[me] = part[me]

    for i in range(tiles):
        own_piece(i, me).wait_send()
    for d in range(1, PEERS):
        send_tgt(d, me).wait_send()

    @pl.when(chip < CHIPS - 1)
    def _():
        hop(me, right, send_r).wait_send()

    @pl.when(chip > 0)
    def _():
        hop(me, left, send_l).wait_send()

    for k in range(1, CHIPS):
        @pl.when(chip >= k)
        def _(k=k):
            b = (me + PEERS - CORES * k) % PEERS
            hop(b, other, send_p).wait_send()

            @pl.when(chip < CHIPS - 1)
            def _():
                hop(b, right, send_r).wait_send()

        @pl.when(chip + k < CHIPS)
        def _(k=k):
            b = (me + CORES * k) % PEERS
            hop(b, other, send_p).wait_send()

            @pl.when(chip > 0)
            def _():
                hop(b, left, send_l).wait_send()

    for d in range(1, PEERS):
        send_stat(d, (me + d) % PEERS, (me + PEERS - d) % PEERS).wait()
    got = [landed[b] for b in range(PEERS)]
    m = _tree(jnp.maximum, [g[0:1] for g in got])
    keep = [jnp.exp(g[0:1] - m) for g in got]
    s = _tree(jnp.add, [g[1:2] * k for g, k in zip(got, keep)])
    w = _tree(jnp.add, [g[2:3] * k for g, k in zip(got, keep)])
    lse = m + jnp.log(s)
    out_ref[0:1, :] = _tree(jnp.add, [g[3:4] for g in got]) - lse
    out_ref[1:2, :] = lse - w / s


def solution(mesh):
    def device_body(h, targets, gain, head, tau):
        tok, depth = h.shape[1:]
        vocab = head.shape[0]
        width = CORES * tok
        anywhere = pl.BlockSpec(memory_space=pl.ANY)
        vmem = pl.BlockSpec(memory_space=pltpu.VMEM)
        dma = pltpu.SemaphoreType.DMA
        stat = pltpu.VMEM((8, (CHIPS + 1) * width), F32)
        out = pl.pallas_call(
            functools.partial(_kernel, tok, vocab, depth),
            out_shape=jax.ShapeDtypeStruct((2, tok), F32),
            in_specs=[pl.BlockSpec(memory_space=pltpu.SMEM), anywhere, anywhere, vmem, anywhere],
            out_specs=vmem,
            scratch_shapes=[
                pltpu.VMEM((PEERS * tok // LANES, depth, LANES), jnp.bfloat16),
                pltpu.VMEM((2, sum(SPLITS), depth), jnp.bfloat16),
                *[pltpu.VMEM((r, width), F32) for r in SPLITS],
                pltpu.VMEM((1, (CHIPS + 1) * width), jnp.int32),
                stat, stat, stat, stat,
                pltpu.VMEM((PEERS, 4, tok), F32),
                pltpu.VMEM((PEERS, 4, tok), F32),
                dma((tok // LANES,)), dma, dma((2,)), dma((tok // LANES,)), dma((tok // LANES,)),
                dma((PEERS,)), dma((PEERS,)), dma((PEERS,)), dma((PEERS,)),
                dma((PEERS,)), dma((PEERS,)), dma((PEERS,)), dma((PEERS,)),
            ],
            compiler_params=pltpu.CompilerParams(
                collective_id=0, has_side_effects=True, vmem_limit_bytes=67_043_328),
        )(tau.reshape(1), h.reshape(tok, depth), targets, gain, head)
        return out[0:1], out[1:2]

    return jax.shard_map(
        device_body,
        mesh=mesh,
        in_specs=(P('dp', 'tp', None), P('dp', 'tp'), P(), P('tp', None), P()),
        out_specs=(P('dp', 'tp'), P('dp', 'tp')),
        check_vma=False,
    )
```
